32 devices in a mesh: cls: 4 (over y, x), org: 8 (over z, core).
Axes of the slice: x: 2, y: 2, z: 4, core: 2. Of those that a mesh axis runs over, the one named last changes fastest.
Arguments:
- flows_start: float32 [8, 49152], P('cls', 'org'), may hold values from 150 to 300
- interaction: float32 [8, 8, 49152], P('cls', None, 'org'), may hold values from 0.2 to 2
- free_time: float32 [8, 49152], P('cls', 'org'), may hold values from 0.01 to 0.1
- capacity: float32 [49152], P('org'), may hold values from 300 to 900
- demand: int32 [8, 8, 60], P('cls', 'org'), may hold values from 0 to 15
- incidence: int32 [2, 8, 8, 2, 49152], P(None, 'cls', 'org'), may hold values from 0 to 1073741823, as said below
- step_size: float32 [2], replicated, may hold values from 0.3 to 0.6
Outputs:
- flows: float32 [8, 49152], P('cls', 'org')
- costs: float32 [8, 49152], P('cls', 'org')
- skims: float32 [2, 8, 8, 60], P(None, 'cls', 'org')
- gaps: float32 [2], replicated
The draws below stay inside these ranges and needn't reach their ends.
Inputs may be any that keep to these rules, and one draw needn't show every extreme that they name: Bit b of incidence[k, c, o, w, l] tells whether link l lies on class c's path from anchor o to destination w * 30 + b in iteration k; each path is the union of 4 runs of 64 consecutive links (counted cyclically over the links) at drawn starts, the first of which is shared by all 30 destinations of one word.
All inputs are finite; a program needn't handle non-finite values.
Results may differ from the reference program's by a relative error of at most 0.0013.
Values sent between devices are 32-bit elements; how exact they have to be, the bound alone decides.
No kernel may reach another device: no remote copies, remote signals or barrier semaphores. Data moves between devices by JAX's collectives and lax.ppermute only.
A program may use at most 256 MiB of HBM per device.

```python
import math
import jax
import jax.numpy as jnp
from jax import lax

C = 8
BITS = 30
DWORDS = 2
LINK_DEV = 6144
ITERS = 2
RUNS = 4
SEG = 64
ANCHORS = 8
DEST = 60
LINKS = 49152
N_ORG = 8


def draw_incidence(key, part):
    own_starts = jax.random.randint(jax.random.fold_in(key, 11), (BITS, ITERS, C, ANCHORS, DWORDS, RUNS - 1), 0, LINKS).astype(jnp.int32)
    shared = jax.random.randint(jax.random.fold_in(key, 23), (1, ITERS, C, ANCHORS, DWORDS, 1), 0, LINKS).astype(jnp.int32)
    shared_all = jnp.broadcast_to(shared, (BITS, ITERS, C, ANCHORS, DWORDS, 1))
    starts = jnp.concatenate([shared_all, own_starts], axis=-1)
    link_ids = jnp.arange(LINKS, dtype=jnp.int32)

    def add_bit(bit_number, words):
        chosen = lax.dynamic_index_in_dim(starts, bit_number, 0, keepdims=False)
        inside = jnp.zeros(words.shape, jnp.bool_)
        for run_index in range(RUNS):
            offset = jnp.mod(link_ids - chosen[..., run_index, None], LINKS)
            inside = jnp.logical_or(inside, offset < SEG)
        return words + jnp.left_shift(inside.astype(jnp.int32), bit_number)
    empty = jnp.zeros((ITERS, C, ANCHORS, DWORDS, LINKS), jnp.int32)
    return lax.fori_loop(0, BITS, add_bit, empty)


def plant(result, rng, low, top_value):
    place = [jax.random.randint(jax.random.fold_in(rng, axis), (), 0, length) for axis, length in enumerate(result.shape)]
    widest = result.shape.index(max(result.shape))
    next_to = place[:widest] + [(place[widest] + 1) % result.shape[widest]] + place[widest + 1:]
    return result.at[tuple(place)].set(low).at[tuple(next_to)].set(top_value)


def shard_levels(own_key, dims, split, low, top_value):
    factor_of = 1.0
    for position, shards_of in split:
        draws = jax.random.uniform(jax.random.fold_in(jax.random.fold_in(own_key, 6), position), (shards_of,), jnp.float32, low / len(split), top_value / len(split))
        factor_of = factor_of * jnp.repeat(jnp.exp(draws), dims[position] // shards_of).reshape((-1,) + (1,) * (len(dims) - 1 - position))
    return factor_of


def setup_inputs(seed: int = 0) -> dict:
    seeds = jax.random.split(jax.random.key(seed), 8)
    return {
        "flows_start": jnp.clip(150.0 + 150.0 * jax.random.uniform(seeds[0], (C, LINKS), jnp.float32) ** shard_levels(seeds[0], (C, LINKS), ((0, 4), (1, 8)), -0.2, 0.2), 150.0, 300.0),
        "interaction": jnp.clip(jnp.exp(math.log(2.0) - 2.3025851 * jax.random.uniform(seeds[1], (C, C, LINKS), jnp.float32) ** shard_levels(seeds[1], (C, C, LINKS), ((0, 4), (2, 8)), -0.2, 0.2)), 0.2, 2.0),
        "free_time": jnp.clip(jnp.exp(math.log(0.1) - 2.3025851 * jax.random.uniform(seeds[2], (C, LINKS), jnp.float32) ** shard_levels(seeds[2], (C, LINKS), ((0, 4), (1, 8)), -0.2, 0.2)), 0.01, 0.1),
        "capacity": jnp.clip(300.0 + 600.0 * jax.random.uniform(seeds[3], (LINKS,), jnp.float32) ** shard_levels(seeds[3], (LINKS,), ((0, 8),), -0.2, 0.2), 300.0, 900.0),
        "demand": plant(jax.random.randint(seeds[4], (C, ANCHORS, DEST), 0, 16), jax.random.fold_in(seeds[4], 1), 0, 15).astype(jnp.int32),
        "incidence": draw_incidence(jax.random.fold_in(seeds[7], 71), 0),
        "step_size": jnp.clip(jax.random.uniform(seeds[6], (ITERS,), jnp.float32, 0.3, 0.6), 0.3, 0.6),
    }


HIGH = lax.Precision.HIGHEST


def unpack(packed):
    shifts = jnp.arange(BITS, dtype=jnp.int32)
    bit_table = jnp.bitwise_and(jnp.right_shift(packed[..., :, None, :], shifts[:, None]), 1)
    new_shape = packed.shape[:-2] + (packed.shape[-2] * BITS, packed.shape[-1])
    return bit_table.reshape(new_shape).astype(jnp.float32)


def link_cost(flows_all, inter, free, cap):
    load_sum = jnp.einsum("cel,el->cl", inter, flows_all, precision=HIGH)
    load_ratio = load_sum / cap
    square = load_ratio * load_ratio
    return free * (1.0 + 0.15 * square * square)


def reference(flows_start, interaction, free_time, capacity, demand, incidence, step_size):
    demand_real = demand.astype(jnp.float32)
    flow_now = flows_start
    skim_list = []
    gap_list = []
    for iteration in range(ITERS):
        cost_now = link_cost(flow_now, interaction, free_time, capacity)
        skim_rows = []
        load_rows = []
        for class_index in range(C):
            packed_all = incidence[iteration, class_index]
            times_row = cost_now[class_index]
            trips = demand_real[class_index]

            def advance(skim_sum, block_index):
                first = block_index * LINK_DEV
                word_block = lax.dynamic_slice_in_dim(packed_all, first, LINK_DEV, 2)
                bit_table = unpack(word_block)
                cost_block = lax.dynamic_slice_in_dim(times_row, first, LINK_DEV, 0)
                skim_sum = skim_sum + jnp.einsum("odl,l->od", bit_table, cost_block, precision=HIGH)
                load_block = jnp.einsum("od,odl->l", trips, bit_table, precision=HIGH)
                return skim_sum, load_block

            skim_sum, load_blocks = lax.scan(advance, jnp.zeros((ANCHORS, DEST), jnp.float32), jnp.arange(N_ORG, dtype=jnp.int32))
            skim_rows.append(skim_sum)
            load_rows.append(load_blocks.reshape(LINKS))
        skim_now = jnp.stack(skim_rows)
        aon = jnp.stack(load_rows)
        cost_total = jnp.sum(cost_now * flow_now)
        path_total = jnp.sum(demand_real * skim_now)
        gap_list.append((cost_total - path_total) / cost_total)
        skim_list.append(skim_now)
        flow_now = flow_now + step_size[iteration] * (aon - flow_now)
    cost_final = link_cost(flow_now, interaction, free_time, capacity)
    return flow_now, cost_final, jnp.stack(skim_list), jnp.stack(gap_list)
```

```python
import jax
import jax.numpy as jnp
from jax import lax
from jax.experimental import pallas as pl
from jax.experimental.pallas import tpu as pltpu
from jax.sharding import PartitionSpec as P

BITS = 30
PLANES = 4
LANES = 128
ROWS = 8
UNROLL = 2


def skim_kernel(words_ref, cost_ref, out_ref):
    steps = words_ref.shape[1] // (ROWS * UNROLL)

    def advance(step, sums):
        sums = list(sums)
        for part in range(UNROLL):
            start = pl.multiple_of((step * UNROLL + part) * ROWS, ROWS)
            words = words_ref[0, pl.ds(start, ROWS), :]
            costs = cost_ref[0, pl.ds(start, ROWS), :]
            for bit in range(BITS):
                chosen = jnp.bitwise_and(words, jnp.int32(1 << bit)) != 0
                sums[bit] = sums[bit] + jnp.where(chosen, costs, 0.0)
        return tuple(sums)

    zero = jnp.zeros((ROWS, LANES), jnp.float32)
    sums = lax.fori_loop(0, steps, advance, (zero,) * BITS)
    lane = lax.broadcasted_iota(jnp.int32, (ROWS, LANES), 1)
    out = zero
    for bit in range(BITS):
        total = jnp.sum(sums[bit], axis=1, keepdims=True)
        out = jnp.where(lane == bit, total, out)
    out_ref[0] = out


def path_costs(words, costs, anchors):
    groups, rows, lanes = words.shape
    return pl.pallas_call(
        skim_kernel,
        grid=(groups,),
        in_specs=[
            pl.BlockSpec((1, rows, lanes), lambda g: (g, 0, 0)),
            pl.BlockSpec((1, rows, lanes), lambda g: (g // anchors, 0, 0)),
        ],
        out_specs=pl.BlockSpec((1, ROWS, LANES), lambda g: (g, 0, 0)),
        out_shape=jax.ShapeDtypeStruct((groups, ROWS, LANES), jnp.float32),
        name="path_costs",
    )(words, costs)


def link_cost(flows_all, inter, free, cap):
    load_sum = jnp.sum(inter * flows_all[None], axis=1)
    load_ratio = load_sum / cap
    square = load_ratio * load_ratio
    return free * (1.0 + 0.15 * square * square)


def own_loads(demand, incidence):
    classes, anchors, dests = demand.shape
    by_word = demand.reshape(classes, anchors, dests // BITS, BITS)
    shifts = jnp.arange(BITS, dtype=jnp.int32)
    total = 0
    for plane in range(PLANES):
        bits = jnp.bitwise_and(jnp.right_shift(by_word, plane), 1)
        mask = jnp.sum(jnp.left_shift(bits, shifts), axis=-1)
        count = lax.population_count(jnp.bitwise_and(incidence, mask[None, ..., None]))
        total = total + jnp.left_shift(count, plane)
    return jnp.sum(total, axis=(2, 3)).astype(jnp.float32)


def shards(flows_start, interaction, free_time, capacity, demand, incidence, step_size):
    orgs = lax.axis_size("org")
    iters, classes, anchors, dwords, links = incidence.shape
    own = flows_start.shape[1]
    blocks = links // LANES

    partial = own_loads(demand, incidence)
    spread = jnp.moveaxis(partial.reshape(iters, classes, orgs, own), 2, 0)
    received = lax.all_to_all(spread, "org", 0, 0)
    aon = jnp.sum(received, axis=0)

    state = jnp.concatenate([flows_start[None], aon], axis=0)
    state_all = lax.all_gather(state, "cls", axis=1, tiled=True)
    flow_all = state_all[0]
    flow_own = flows_start
    cost_list = []
    totals = []
    for k in range(iters):
        cost = link_cost(flow_all, interaction, free_time, capacity)
        cost_list.append(cost)
        totals.append(jnp.sum(cost * flow_own))
        totals.append(jnp.sum(cost * aon[k]))
        flow_all = flow_all + step_size[k] * (state_all[k + 1] - flow_all)
        flow_own = flow_own + step_size[k] * (aon[k] - flow_own)
    cost_final = link_cost(flow_all, interaction, free_time, capacity)

    costs = jnp.stack(cost_list)
    costs_all = lax.all_gather(costs, "org", axis=2, tiled=True)
    sums = lax.psum(jnp.stack(totals), ("cls", "org")).reshape(iters, 2)
    gaps = (sums[:, 0] - sums[:, 1]) / sums[:, 0]

    groups = iters * classes * anchors
    words = incidence.reshape(iters, classes, anchors, dwords, blocks, LANES)
    words = jnp.swapaxes(words, 3, 4).reshape(groups, blocks * dwords, LANES)
    wide = costs_all.reshape(iters * classes, blocks, 1, LANES)
    wide = jnp.broadcast_to(wide, (iters * classes, blocks, dwords, LANES))
    wide = wide.reshape(iters * classes, blocks * dwords, LANES)
    found = path_costs(words, wide, anchors)
    found = found.reshape(groups, ROWS // dwords, dwords, LANES).sum(1)
    skims = found[:, :, :BITS].reshape(iters, classes, anchors, dwords * BITS)
    return (flow_own, cost_final, skims, gaps)


def solution(mesh):
    placed = (
        P("cls", "org"),
        P("cls", None, "org"),
        P("cls", "org"),
        P("org"),
        P("cls", "org", None),
        P(None, "cls", "org", None, None),
        P(),
    )
    return jax.shard_map(
        shards,
        mesh=mesh,
        in_specs=placed,
        out_specs=(P("cls", "org"), P("cls", "org"), P(None, "cls", "org", None), P()),
        check_vma=False,
    )
```

```python
import jax
import jax.numpy as jnp
from jax import lax
from jax.experimental import pallas as pl
from jax.experimental.pallas import tpu as pltpu
from jax.sharding import PartitionSpec as P

BITS = 30
PLANES = 4
LANES = 128
ROWS = 8


def load_kernel(mask_ref, words_ref, out_ref):
    pairs, masks = mask_ref.shape
    dwords = masks // PLANES
    pair = pl.program_id(0) % pairs
    mask = [mask_ref[pair, m] for m in range(masks)]

    def step(index, carry):
        start = pl.multiple_of(index * ROWS, ROWS)
        total = jnp.zeros((ROWS, LANES), jnp.int32)
        for word in range(dwords):
            bits = words_ref[0, pl.ds(start * dwords + word, ROWS, stride=dwords), :]
            for plane in range(PLANES):
                count = lax.population_count(jnp.bitwise_and(bits, mask[plane * dwords + word]))
                total = total + jnp.left_shift(count, plane)
        out_ref[0, pl.ds(start, ROWS), :] = total.astype(jnp.float32)
        return carry

    lax.fori_loop(0, out_ref.shape[1] // ROWS, step, 0, unroll=4)


def own_loads(words, masks, dwords):
    groups, rows, lanes = words.shape
    return pl.pallas_call(
        load_kernel,
        grid=(groups,),
        in_specs=[
            pl.BlockSpec(memory_space=pltpu.SMEM),
            pl.BlockSpec((1, rows, lanes), lambda g: (g, 0, 0)),
        ],
        out_specs=pl.BlockSpec((1, rows // dwords, lanes), lambda g: (g, 0, 0)),
        out_shape=jax.ShapeDtypeStruct((groups, rows // dwords, lanes), jnp.float32),
        name="own_loads",
    )(masks, words)


def demand_masks(demand, dwords):
    classes, anchors, dests = demand.shape
    by_word = demand.reshape(classes * anchors, 1, dwords, BITS)
    planes = jnp.arange(PLANES, dtype=jnp.int32)[:, None, None]
    bits = jnp.bitwise_and(jnp.right_shift(by_word, planes), 1)
    mask = jnp.sum(jnp.left_shift(bits, jnp.arange(BITS, dtype=jnp.int32)), axis=-1)
    return mask.reshape(classes * anchors, PLANES * dwords)


def skim_kernel(place_ref, words_ref, cost_ref, out_ref):
    pieces, _, blocks, _ = cost_ref.shape
    dwords = out_ref.shape[1] // ROWS
    lane = lax.broadcasted_iota(jnp.int32, (ROWS, LANES), 1)
    zero = jnp.zeros((ROWS, LANES), jnp.float32)
    for word in range(dwords):

        def advance(piece, sums):
            sums = list(sums)
            base = place_ref[piece] * blocks
            for chunk in range(blocks // ROWS):
                start = (base + chunk * ROWS) * dwords + word
                words = words_ref[0, pl.ds(start, ROWS, stride=dwords), :]
                costs = cost_ref[piece, 0, chunk * ROWS:(chunk + 1) * ROWS, :]
                for bit in range(BITS):
                    chosen = jnp.bitwise_and(words, jnp.int32(1 << bit)) != 0
                    sums[bit] = sums[bit] + jnp.where(chosen, costs, 0.0)
            return tuple(sums)

        sums = lax.fori_loop(0, pieces, advance, (zero,) * BITS)
        out = zero
        for bit in range(BITS):
            total = jnp.sum(sums[bit], axis=1, keepdims=True)
            out = jnp.where(lane == bit, total, out)
        out_ref[0, word * ROWS:(word + 1) * ROWS, :] = out


def path_costs(words, costs, places, iteration, anchors, dwords):
    pieces, classes, blocks, lanes = costs.shape
    rows = words.shape[1]
    groups = classes * anchors
    out = pl.pallas_call(
        skim_kernel,
        grid=(groups,),
        in_specs=[
            pl.BlockSpec(memory_space=pltpu.SMEM),
            pl.BlockSpec((1, rows, lanes), lambda g: (iteration * groups + g, 0, 0)),
            pl.BlockSpec((pieces, 1, blocks, lanes), lambda g: (0, g // anchors, 0, 0)),
        ],
        out_specs=pl.BlockSpec((1, dwords * ROWS, LANES), lambda g: (g, 0, 0)),
        out_shape=jax.ShapeDtypeStruct((groups, dwords * ROWS, LANES), jnp.float32),
        name="path_costs",
    )(places, words, costs)
    return out.reshape(classes, anchors, dwords, ROWS, LANES)


def swap(value, axis, mask):
    size = lax.axis_size(axis)
    return lax.ppermute(value, axis, [(i, i ^ mask) for i in range(size)])


def link_cost(flow_pieces, inter_pieces, free, cap):
    load_sum = 0.0
    for flow, inter in zip(flow_pieces, inter_pieces):
        for e in range(flow.shape[0]):
            load_sum = load_sum + inter[:, e] * flow[e][None]
    load_ratio = load_sum / cap
    square = load_ratio * load_ratio
    return free * (1.0 + 0.15 * square * square)


def mesh_sum(value):
    for axis in ("org", "cls"):
        mask = 1
        while mask < lax.axis_size(axis):
            value = value + swap(value, axis, mask)
            mask *= 2
    return value


def shards(flows_start, interaction, free_time, capacity, demand, incidence, step_size):
    orgs = lax.axis_size("org")
    sets = lax.axis_size("cls")
    half = orgs // 2
    org = lax.axis_index("org")
    cls = lax.axis_index("cls")
    iters, classes, anchors, dwords, links = incidence.shape
    own = flows_start.shape[1]
    blocks = own // LANES
    groups = iters * classes * anchors

    words = incidence.reshape(groups, dwords, links // LANES, LANES)
    words = jnp.swapaxes(words, 1, 2).reshape(groups, links // LANES * dwords, LANES)
    flow_own = flows_start.reshape(classes, blocks, LANES)
    free = free_time.reshape(classes, blocks, LANES)
    cap = capacity.reshape(blocks, LANES)
    inter = interaction.reshape(classes, sets, classes, blocks, LANES)
    inter_pieces = [
        lax.dynamic_index_in_dim(inter, jnp.bitwise_xor(cls, s), 1, keepdims=False) for s in range(sets)
    ]

    partial = own_loads(words, demand_masks(demand, dwords), dwords)
    partial = partial.reshape(iters, classes, anchors, half, 2, blocks, LANES).sum(2)
    core = jnp.bitwise_and(org, 1)
    for_mine = lax.dynamic_index_in_dim(partial, core, 3, keepdims=False)
    for_other = lax.dynamic_index_in_dim(partial, 1 - core, 3, keepdims=False)
    chip = for_mine + swap(for_other, "org", 1)
    spot = jnp.right_shift(org, 1)
    aon = lax.dynamic_index_in_dim(chip, spot, 2, keepdims=False)
    for t in range(1, half):
        leaving = lax.dynamic_index_in_dim(chip, jnp.bitwise_xor(spot, t), 2, keepdims=False)
        aon = aon + swap(leaving, "org", 2 * t)

    flow_pieces = [flow_own] + [swap(flow_own, "cls", s) for s in range(1, sets)]
    aon_pieces = [aon] + [swap(aon, "cls", s) for s in range(1, sets)]

    reach = jnp.arange(half, dtype=jnp.int32) * 2
    near = jnp.bitwise_xor(org, reach)
    far = jnp.bitwise_xor(near, 1)
    totals = []
    skims = []
    for k in range(iters):
        cost = link_cost(flow_pieces, inter_pieces, free, cap)
        mine = jnp.stack([cost] + [swap(cost, "org", 2 * t) for t in range(1, half)])
        other = swap(mine, "org", 1)
        found = path_costs(words, mine, near, k, anchors, dwords)
        found = found + path_costs(words, other, far, k, anchors, dwords)
        found = found.sum(3)[..., :BITS].reshape(classes, anchors, dwords * BITS)
        skims.append(found)
        totals.append(jnp.sum(cost * flow_pieces[0]))
        totals.append(jnp.sum(cost * aon[k]))
        flow_pieces = [f + step_size[k] * (a[k] - f) for f, a in zip(flow_pieces, aon_pieces)]
    cost_final = link_cost(flow_pieces, inter_pieces, free, cap)
    sums = mesh_sum(jnp.stack(totals)).reshape(iters, 2)
    gaps = (sums[:, 0] - sums[:, 1]) / sums[:, 0]
    return (
        flow_pieces[0].reshape(classes, own),
        cost_final.reshape(classes, own),
        jnp.stack(skims),
        gaps,
    )


def solution(mesh):
    placed = (
        P("cls", "org"),
        P("cls", None, "org"),
        P("cls", "org"),
        P("org"),
        P("cls", "org", None),
        P(None, "cls", "org", None, None),
        P(),
    )
    return jax.shard_map(
        shards,
        mesh=mesh,
        in_specs=placed,
        out_specs=(P("cls", "org"), P("cls", "org"), P(None, "cls", "org", None), P()),
        check_vma=False,
    )
```

```python
import functools

import jax
import jax.numpy as jnp
from jax import lax
from jax.experimental import pallas as pl
from jax.experimental.pallas import tpu as pltpu
from jax.sharding import PartitionSpec as P

BITS = 30
PLANES = 4
LANES = 128
ROWS = 8


def load_kernel(mask_ref, words_ref, out_ref):
    pairs, masks = mask_ref.shape
    dwords = masks // PLANES
    pair = pl.program_id(0) % pairs
    mask = [mask_ref[pair, m] for m in range(masks)]

    def step(index, carry):
        start = pl.multiple_of(index * ROWS, ROWS)
        total = jnp.zeros((ROWS, LANES), jnp.int32)
        for word in range(dwords):
            bits = words_ref[0, pl.ds(start * dwords + word, ROWS, stride=dwords), :]
            for plane in range(PLANES):
                count = lax.population_count(jnp.bitwise_and(bits, mask[plane * dwords + word]))
                total = total + jnp.left_shift(count, plane)
        out_ref[0, pl.ds(start, ROWS), :] = total.astype(jnp.float32)
        return carry

    lax.fori_loop(0, out_ref.shape[1] // ROWS, step, 0, unroll=4)


def own_loads(words, masks, dwords):
    groups, rows, lanes = words.shape
    return pl.pallas_call(
        load_kernel,
        grid=(groups,),
        in_specs=[
            pl.BlockSpec(memory_space=pltpu.SMEM),
            pl.BlockSpec((1, rows, lanes), lambda g: (g, 0, 0)),
        ],
        out_specs=pl.BlockSpec((1, rows // dwords, lanes), lambda g: (g, 0, 0)),
        out_shape=jax.ShapeDtypeStruct((groups, rows // dwords, lanes), jnp.float32),
        name="own_loads",
    )(masks, words)


def demand_masks(demand, dwords):
    classes, anchors, dests = demand.shape
    by_word = demand.reshape(classes * anchors, 1, dwords, BITS)
    planes = jnp.arange(PLANES, dtype=jnp.int32)[:, None, None]
    bits = jnp.bitwise_and(jnp.right_shift(by_word, planes), 1)
    mask = jnp.sum(jnp.left_shift(bits, jnp.arange(BITS, dtype=jnp.int32)), axis=-1)
    return mask.reshape(classes * anchors, PLANES * dwords)


def skim_kernel(first, anchors, blocks, place_ref, words_ref, *refs):
    cost_refs, out_ref = refs[:-1], refs[-1]
    dwords = out_ref.shape[1] // ROWS
    row = ((first + pl.program_id(0)) // anchors) * blocks
    lane = lax.broadcasted_iota(jnp.int32, (ROWS, LANES), 1)
    zero = jnp.zeros((ROWS, LANES), jnp.float32)
    for word in range(dwords):

        def advance(chunk, sums):
            sums = list(sums)
            shift = pl.multiple_of(chunk * ROWS, ROWS)
            for piece, cost_ref in enumerate(cost_refs):
                start = (place_ref[piece] * blocks + shift) * dwords + word
                words = words_ref[0, pl.ds(start, ROWS, stride=dwords), :]
                costs = cost_ref[pl.ds(pl.multiple_of(row + shift, ROWS), ROWS), :]
                for bit in range(BITS):
                    chosen = jnp.bitwise_and(words, jnp.int32(1 << bit)) != 0
                    sums[bit] = sums[bit] + jnp.where(chosen, costs, 0.0)
            return tuple(sums)

        sums = lax.fori_loop(0, blocks // ROWS, advance, (zero,) * BITS)
        out = zero
        for bit in range(BITS):
            total = jnp.sum(sums[bit], axis=1, keepdims=True)
            out = jnp.where(lane == bit, total, out)
        out_ref[0, word * ROWS:(word + 1) * ROWS, :] = out


def path_costs(words, pieces, places, first, count, anchors, blocks, dwords):
    rows = words.shape[1]
    kernel = functools.partial(skim_kernel, first, anchors, blocks)
    whole = pl.BlockSpec(pieces[0].shape, lambda g: (0, 0))
    return pl.pallas_call(
        kernel,
        grid=(count,),
        in_specs=[
            pl.BlockSpec(memory_space=pltpu.SMEM),
            pl.BlockSpec((1, rows, LANES), lambda g: (first + g, 0, 0)),
        ] + [whole] * len(pieces),
        out_specs=pl.BlockSpec((1, dwords * ROWS, LANES), lambda g: (g, 0, 0)),
        out_shape=jax.ShapeDtypeStruct((count, dwords * ROWS, LANES), jnp.float32),
        cost_estimate=pl.CostEstimate(
            flops=count * 500_000_000, transcendentals=0, bytes_accessed=count * rows * LANES * 4
        ),
        name="path_costs",
    )(places, words, *pieces)


def link_kernel(step_ref, cls_ref, *refs):
    sets = (len(refs) - 6) // 2
    flow_refs, aon_refs = refs[:sets], refs[sets:2 * sets]
    inter_ref, free_ref, cap_ref, pay_ref, flow_out, cost_out = refs[2 * sets:]
    classes, blocks, _ = free_ref.shape
    iters = aon_refs[0].shape[0]
    sources = [cls_ref[0] ^ s for s in range(sets)]

    def cost_of(flows, c, rows):
        load = jnp.zeros((ROWS, LANES), jnp.float32)
        for s in range(sets):
            for e in range(classes):
                load = load + inter_ref[c, sources[s] * classes + e, rows, :] * flows[s][e]
        ratio = load / cap_ref[rows, :]
        square = ratio * ratio
        return free_ref[c, rows, :] * (1.0 + 0.15 * square * square)

    def step(index, totals):
        totals = list(totals)
        start = pl.multiple_of(index * ROWS, ROWS)
        rows = pl.ds(start, ROWS)
        flows = [[ref[e, rows, :] for e in range(classes)] for ref in flow_refs]
        for k in range(iters):
            loads = [[ref[k, e, rows, :] for e in range(classes)] for ref in aon_refs]
            for c in range(classes):
                cost = cost_of(flows, c, rows)
                place = pl.multiple_of((k * classes + c) * blocks + start, ROWS)
                pay_ref[pl.ds(place, ROWS), :] = cost
                totals[2 * k] = totals[2 * k] + cost * flows[0][c]
                totals[2 * k + 1] = totals[2 * k + 1] + cost * loads[0][c]
            size = step_ref[k]
            flows = [[f + size * (a - f) for f, a in zip(fs, ls)] for fs, ls in zip(flows, loads)]
        for c in range(classes):
            flow_out[c, rows, :] = flows[0][c]
            cost_out[c, rows, :] = cost_of(flows, c, rows)
        return tuple(totals)

    zero = jnp.zeros((ROWS, LANES), jnp.float32)
    totals = lax.fori_loop(0, blocks // ROWS, step, (zero,) * (2 * iters))
    rank = lax.broadcasted_iota(jnp.int32, (ROWS, LANES), 0)
    out = zero
    for index, total in enumerate(totals):
        out = jnp.where(rank == index, jnp.sum(total, axis=0, keepdims=True), out)
    pay_ref[iters * classes * blocks:, :] = out


def link_times(step_size, cls, flow_pieces, aon_pieces, inter, free, cap):
    classes, blocks, lanes = free.shape
    iters = aon_pieces[0].shape[0]
    smem = pl.BlockSpec(memory_space=pltpu.SMEM)
    vmem = pl.BlockSpec(memory_space=pltpu.VMEM)
    own = jax.ShapeDtypeStruct(free.shape, jnp.float32)
    payload = jax.ShapeDtypeStruct((iters * classes * blocks + ROWS, lanes), jnp.float32)
    return pl.pallas_call(
        link_kernel,
        in_specs=[smem, smem] + [vmem] * (len(flow_pieces) + len(aon_pieces) + 3),
        out_specs=[vmem] * 3,
        out_shape=[payload, own, own],
        name="link_times",
    )(step_size, cls[None], *flow_pieces, *aon_pieces, inter, free, cap)


def swap(value, axis, mask):
    size = lax.axis_size(axis)
    return lax.ppermute(value, axis, [(i, i ^ mask) for i in range(size)])


def tree_sum(values):
    while len(values) > 1:
        values = [x + y for x, y in zip(values[::2], values[1::2])]
    return values[0]


def shards(flows_start, interaction, free_time, capacity, demand, incidence, step_size):
    orgs = lax.axis_size("org")
    sets = lax.axis_size("cls")
    half = orgs // 2
    org = lax.axis_index("org")
    cls = lax.axis_index("cls")
    iters, classes, anchors, dwords, links = incidence.shape
    own = flows_start.shape[1]
    blocks = own // LANES
    groups = iters * classes * anchors

    words = incidence.reshape(groups, dwords, links // LANES, LANES)
    words = jnp.swapaxes(words, 1, 2).reshape(groups, links // LANES * dwords, LANES)
    flow_own = flows_start.reshape(classes, blocks, LANES)
    free = free_time.reshape(classes, blocks, LANES)
    cap = capacity.reshape(blocks, LANES)
    inter = interaction.reshape(classes, sets * classes, blocks, LANES)

    partial = own_loads(words, demand_masks(demand, dwords), dwords)
    partial = partial.reshape(iters, classes, anchors, half, 2, blocks, LANES).sum(2)
    core = jnp.bitwise_and(org, 1)
    for_mine = lax.dynamic_index_in_dim(partial, core, 3, keepdims=False)
    for_other = lax.dynamic_index_in_dim(partial, 1 - core, 3, keepdims=False)
    chip = for_mine + swap(for_other, "org", 1)
    spot = jnp.right_shift(org, 1)
    aon = lax.dynamic_index_in_dim(chip, spot, 2, keepdims=False)
    for t in range(1, half):
        leaving = lax.dynamic_index_in_dim(chip, jnp.bitwise_xor(spot, t), 2, keepdims=False)
        aon = aon + swap(leaving, "org", 2 * t)

    flow_pieces = [flow_own] + [swap(flow_own, "cls", s) for s in range(1, sets)]
    aon_pieces = [aon] + [swap(aon, "cls", s) for s in range(1, sets)]

    payload, flow_out, cost_out = link_times(step_size, cls, flow_pieces, aon_pieces, inter, free, cap)

    reach = jnp.arange(half, dtype=jnp.int32) * 2
    near = jnp.bitwise_xor(org, reach)
    far = jnp.bitwise_xor(near, 1)
    mine = [payload] + [swap(payload, "org", 2 * t) for t in range(1, half)]
    other = [swap(piece, "org", 1) for piece in mine]
    split = groups // iters
    shape = (anchors, blocks, dwords)
    found = path_costs(words, mine, near, 0, groups, *shape)
    tails = [tree_sum([piece[-ROWS:] for piece in part]) for part in (mine, other)]
    sums = jnp.sum(tails[0] + tails[1], axis=1)
    sums = sums + swap(sums, "cls", 1)
    rest = [path_costs(words, other, far, 0, split, *shape)]
    sums, rest[0], far = lax.optimization_barrier((sums, rest[0], far))
    mask = 2
    while mask < sets:
        sums = sums + swap(sums, "cls", mask)
        mask *= 2
    rest.append(path_costs(words, other, far, split, groups - split, *shape))
    found = found + jnp.concatenate(rest, axis=0)
    found = found.reshape(iters, classes, anchors, dwords, ROWS, LANES).sum(4)
    skims = found[..., :BITS].reshape(iters, classes, anchors, dwords * BITS)
    sums = sums[:2 * iters].reshape(iters, 2)
    gaps = (sums[:, 0] - sums[:, 1]) / sums[:, 0]
    return (flow_out.reshape(classes, own), cost_out.reshape(classes, own), skims, gaps)


def solution(mesh):
    placed = (
        P("cls", "org"),
        P("cls", None, "org"),
        P("cls", "org"),
        P("org"),
        P("cls", "org", None),
        P(None, "cls", "org", None, None),
        P(),
    )
    return jax.shard_map(
        shards,
        mesh=mesh,
        in_specs=placed,
        out_specs=(P("cls", "org"), P("cls", "org"), P(None, "cls", "org", None), P()),
        check_vma=False,
    )
```

```python
import functools

import jax
import jax.numpy as jnp
from jax import lax
from jax.experimental import pallas as pl
from jax.experimental.pallas import tpu as pltpu
from jax.sharding import PartitionSpec as P

BITS = 30
PLANES = 4
LANES = 128
ROWS = 8


def load_kernel(demand_ref, words_ref, out_ref):
    pairs, dests = demand_ref.shape
    dwords = dests // BITS
    pair = pl.program_id(0) % pairs
    mask = [jnp.int32(0)] * (PLANES * dwords)
    for dest in range(dests):
        trips = demand_ref[pair, dest]
        word, bit = divmod(dest, BITS)
        for plane in range(PLANES):
            chosen = jnp.left_shift(jnp.bitwise_and(jnp.right_shift(trips, plane), 1), bit)
            mask[plane * dwords + word] = jnp.bitwise_or(mask[plane * dwords + word], chosen)

    def step(index, carry):
        start = pl.multiple_of(index * ROWS, ROWS)
        total = jnp.zeros((ROWS, LANES), jnp.int32)
        for word in range(dwords):
            bits = words_ref[0, pl.ds(start * dwords + word, ROWS, stride=dwords), :]
            for plane in range(PLANES):
                count = lax.population_count(jnp.bitwise_and(bits, mask[plane * dwords + word]))
                total = total + jnp.left_shift(count, plane)
        out_ref[0, pl.ds(start, ROWS), :] = total.astype(jnp.float32)
        return carry

    lax.fori_loop(0, out_ref.shape[1] // ROWS, step, 0, unroll=4)


def own_loads(words, trips, dwords):
    groups, rows, lanes = words.shape
    return pl.pallas_call(
        load_kernel,
        grid=(groups,),
        in_specs=[
            pl.BlockSpec(memory_space=pltpu.SMEM),
            pl.BlockSpec((1, rows, lanes), lambda g: (g, 0, 0)),
        ],
        out_specs=pl.BlockSpec((1, rows // dwords, lanes), lambda g: (g, 0, 0)),
        out_shape=jax.ShapeDtypeStruct((groups, rows // dwords, lanes), jnp.float32),
        name="own_loads",
    )(trips, words)


def skim_kernel(first, anchors, blocks, place_ref, words_ref, *refs):
    cost_refs, out_ref = refs[:-1], refs[-1]
    dwords = out_ref.shape[1] // ROWS
    row = ((first + pl.program_id(0)) // anchors) * blocks
    lane = lax.broadcasted_iota(jnp.int32, (ROWS, LANES), 1)
    zero = jnp.zeros((ROWS, LANES), jnp.float32)
    for word in range(dwords):

        def advance(chunk, sums):
            sums = list(sums)
            shift = pl.multiple_of(chunk * ROWS, ROWS)
            for piece, cost_ref in enumerate(cost_refs):
                start = (place_ref[piece] * blocks + shift) * dwords + word
                words = words_ref[0, pl.ds(start, ROWS, stride=dwords), :]
                costs = cost_ref[pl.ds(pl.multiple_of(row + shift, ROWS), ROWS), :]
                for bit in range(BITS):
                    chosen = jnp.bitwise_and(words, jnp.int32(1 << bit)) != 0
                    sums[bit] = sums[bit] + jnp.where(chosen, costs, 0.0)
            return tuple(sums)

        sums = lax.fori_loop(0, blocks // ROWS, advance, (zero,) * BITS)
        out = zero
        for bit in range(BITS):
            total = jnp.sum(sums[bit], axis=1, keepdims=True)
            out = jnp.where(lane == bit, total, out)
        out_ref[0, word * ROWS:(word + 1) * ROWS, :] = out


def path_costs(words, pieces, places, first, count, anchors, blocks, dwords):
    rows = words.shape[1]
    kernel = functools.partial(skim_kernel, first, anchors, blocks)
    whole = pl.BlockSpec(pieces[0].shape, lambda g: (0, 0))
    return pl.pallas_call(
        kernel,
        grid=(count,),
        in_specs=[
            pl.BlockSpec(memory_space=pltpu.SMEM),
            pl.BlockSpec((1, rows, LANES), lambda g: (first + g, 0, 0)),
        ] + [whole] * len(pieces),
        out_specs=pl.BlockSpec((1, dwords * ROWS, LANES), lambda g: (g, 0, 0)),
        out_shape=jax.ShapeDtypeStruct((count, dwords * ROWS, LANES), jnp.float32),
        cost_estimate=pl.CostEstimate(
            flops=count * 500_000_000, transcendentals=0, bytes_accessed=count * rows * LANES * 4
        ),
        name="path_costs",
    )(places, words, *pieces)


def link_kernel(step_ref, cls_ref, *refs):
    sets = (len(refs) - 6) // 2
    flow_refs, aon_refs = refs[:sets], refs[sets:2 * sets]
    inter_ref, free_ref, cap_ref, pay_ref, flow_out, cost_out = refs[2 * sets:]
    classes, blocks, _ = free_ref.shape
    iters = aon_refs[0].shape[0]
    sources = [cls_ref[0] ^ s for s in range(sets)]

    def cost_of(flows, c, rows):
        load = jnp.zeros((ROWS, LANES), jnp.float32)
        for s in range(sets):
            for e in range(classes):
                load = load + inter_ref[c, sources[s] * classes + e, rows, :] * flows[s][e]
        ratio = load / cap_ref[rows, :]
        square = ratio * ratio
        return free_ref[c, rows, :] * (1.0 + 0.15 * square * square)

    def step(index, totals):
        totals = list(totals)
        start = pl.multiple_of(index * ROWS, ROWS)
        rows = pl.ds(start, ROWS)
        flows = [[ref[e, rows, :] for e in range(classes)] for ref in flow_refs]
        for k in range(iters):
            loads = [[ref[k, e, rows, :] for e in range(classes)] for ref in aon_refs]
            for c in range(classes):
                cost = cost_of(flows, c, rows)
                place = pl.multiple_of((k * classes + c) * blocks + start, ROWS)
                pay_ref[pl.ds(place, ROWS), :] = cost
                totals[2 * k] = totals[2 * k] + cost * flows[0][c]
                totals[2 * k + 1] = totals[2 * k + 1] + cost * loads[0][c]
            size = step_ref[k]
            flows = [[f + size * (a - f) for f, a in zip(fs, ls)] for fs, ls in zip(flows, loads)]
        for c in range(classes):
            flow_out[c, rows, :] = flows[0][c]
            cost_out[c, rows, :] = cost_of(flows, c, rows)
        return tuple(totals)

    zero = jnp.zeros((ROWS, LANES), jnp.float32)
    totals = lax.fori_loop(0, blocks // ROWS, step, (zero,) * (2 * iters))
    rank = lax.broadcasted_iota(jnp.int32, (ROWS, LANES), 0)
    out = zero
    for index, total in enumerate(totals):
        out = jnp.where(rank == index, jnp.sum(total, axis=0, keepdims=True), out)
    pay_ref[iters * classes * blocks:, :] = out


def link_times(step_size, cls, flow_pieces, aon_pieces, inter, free, cap):
    classes, blocks, lanes = free.shape
    iters = aon_pieces[0].shape[0]
    smem = pl.BlockSpec(memory_space=pltpu.SMEM)
    vmem = pl.BlockSpec(memory_space=pltpu.VMEM)
    own = jax.ShapeDtypeStruct(free.shape, jnp.float32)
    payload = jax.ShapeDtypeStruct((iters * classes * blocks + ROWS, lanes), jnp.float32)
    return pl.pallas_call(
        link_kernel,
        in_specs=[smem, smem] + [vmem] * (len(flow_pieces) + len(aon_pieces) + 3),
        out_specs=[vmem] * 3,
        out_shape=[payload, own, own],
        name="link_times",
    )(step_size, cls[None], *flow_pieces, *aon_pieces, inter, free, cap)


def swap(value, axis, mask):
    size = lax.axis_size(axis)
    return lax.ppermute(value, axis, [(i, i ^ mask) for i in range(size)])


def tree_sum(values):
    while len(values) > 1:
        values = [x + y for x, y in zip(values[::2], values[1::2])]
    return values[0]


def shards(flows_start, interaction, free_time, capacity, demand, incidence, step_size):
    orgs = lax.axis_size("org")
    sets = lax.axis_size("cls")
    half = orgs // 2
    org = lax.axis_index("org")
    cls = lax.axis_index("cls")
    iters, classes, anchors, dwords, links = incidence.shape
    own = flows_start.shape[1]
    blocks = own // LANES
    groups = iters * classes * anchors

    words = incidence.reshape(groups, dwords, links // LANES, LANES)
    words = jnp.swapaxes(words, 1, 2).reshape(groups, links // LANES * dwords, LANES)
    flow_own = flows_start.reshape(classes, blocks, LANES)
    free = free_time.reshape(classes, blocks, LANES)
    cap = capacity.reshape(blocks, LANES)
    inter = interaction.reshape(classes, sets * classes, blocks, LANES)

    partial = own_loads(words, demand.reshape(classes * anchors, dwords * BITS), dwords)
    partial = partial.reshape(iters, classes, anchors, half, 2, blocks, LANES).sum(2)
    core = jnp.bitwise_and(org, 1)
    for_mine = lax.dynamic_index_in_dim(partial, core, 3, keepdims=False)
    for_other = lax.dynamic_index_in_dim(partial, 1 - core, 3, keepdims=False)
    chip = for_mine + swap(for_other, "org", 1)
    spot = jnp.right_shift(org, 1)
    aon = lax.dynamic_index_in_dim(chip, spot, 2, keepdims=False)
    for t in range(1, half):
        leaving = lax.dynamic_index_in_dim(chip, jnp.bitwise_xor(spot, t), 2, keepdims=False)
        arrived = swap(leaving, "org", 2 * t)
        if t == 1:
            arrived, flow_own = lax.optimization_barrier((arrived, flow_own))
        aon = aon + arrived

    flow_pieces = [flow_own] + [swap(flow_own, "cls", s) for s in range(1, sets)]
    aon_pieces = [aon] + [swap(aon, "cls", s) for s in range(1, sets)]

    payload, flow_out, cost_out = link_times(step_size, cls, flow_pieces, aon_pieces, inter, free, cap)

    reach = jnp.arange(half, dtype=jnp.int32) * 2
    near = jnp.bitwise_xor(org, reach)
    far = jnp.bitwise_xor(near, 1)
    mine = [payload] + [swap(payload, "org", 2 * t) for t in range(1, half)]
    other = [swap(piece, "org", 1) for piece in mine]
    split = groups // iters
    shape = (anchors, blocks, dwords)
    found = path_costs(words, mine, near, 0, groups, *shape)
    tails = [tree_sum([piece[-ROWS:] for piece in part]) for part in (mine, other)]
    sums = jnp.sum(tails[0] + tails[1], axis=1)
    sums = sums + swap(sums, "cls", 1)
    rest = [path_costs(words, other, far, 0, split, *shape)]
    sums, rest[0], far = lax.optimization_barrier((sums, rest[0], far))
    mask = 2
    while mask < sets:
        sums = sums + swap(sums, "cls", mask)
        mask *= 2
    rest.append(path_costs(words, other, far, split, groups - split, *shape))
    found = found + jnp.concatenate(rest, axis=0)
    found = found.reshape(iters, classes, anchors, dwords, ROWS, LANES).sum(4)
    skims = found[..., :BITS].reshape(iters, classes, anchors, dwords * BITS)
    sums = sums[:2 * iters].reshape(iters, 2)
    gaps = (sums[:, 0] - sums[:, 1]) / sums[:, 0]
    return (flow_out.reshape(classes, own), cost_out.reshape(classes, own), skims, gaps)


def solution(mesh):
    placed = (
        P("cls", "org"),
        P("cls", None, "org"),
        P("cls", "org"),
        P("org"),
        P("cls", "org", None),
        P(None, "cls", "org", None, None),
        P(),
    )
    return jax.shard_map(
        shards,
        mesh=mesh,
        in_specs=placed,
        out_specs=(P("cls", "org"), P("cls", "org"), P(None, "cls", "org", None), P()),
        check_vma=False,
    )
```
